32 devices in a mesh: wide: 8 (over y, x, core), narrow: 4 (over z).
Axes of the slice: x: 2, y: 2, z: 4, core: 2. Of those that a mesh axis runs over, the one named last changes fastest.
Arguments:
- node_features: bfloat16 [2048, 25, 128], P(('wide', 'narrow')), may hold values from -6 to 6
- frames: bfloat16 [2048, 48, 165], P(('wide', 'narrow')), may hold values from -6 to 6
- radial: bfloat16 [2048, 48, 128], P(('wide', 'narrow')), may hold values from 0.29882812 to 3
- neighbours: int32 [2048, 48], P(('wide', 'narrow')), may hold values from 0 to 2047, as said below
- counts: int32 [2048], P(('wide', 'narrow')), may hold values from 16 to 48
- coefficients: float32 [32], P('wide'), may hold values from 0.05 to 0.5
- w_zero: bfloat16 [32, 640, 640], P('wide'), may hold values from -0.25 to 0.25
- w_one: bfloat16 [32, 2, 512, 512], P('wide'), may hold values from -0.1875 to 0.1875
- w_two: bfloat16 [32, 2, 384, 384], P('wide'), may hold values from -0.21875 to 0.21875
- w_three: bfloat16 [32, 2, 256, 256], P('wide'), may hold values from -0.25 to 0.25
- w_four: bfloat16 [32, 2, 128, 128], P('wide'), may hold values from -0.375 to 0.375
Outputs:
- conv_out: float32 [2048, 25, 128], P(('wide', 'narrow'))
The draws below stay inside these ranges and needn't reach their ends.
Inputs may be any that keep to these rules, and one draw needn't show every extreme that they name: `neighbours`: each neighbour of an atom lies in the atom's own aligned block of 64 atoms or in one of the two cyclically adjacent blocks. `counts`: slots at or beyond an atom's count are padding and carry arbitrary indices.
All inputs are finite; a program needn't handle non-finite values.
Results may differ from the reference program's by a relative error of at most 0.02.
Values may be sent and summed in bfloat16 or wider, within the bound.
A program may use at most 192 MiB of HBM per device.

```python
import math
import jax
import jax.numpy as jnp
from jax import lax

C = 128
EXPERTS = 32
NEIGH = 48
ATOM_DEV = 64
ATOMS = 2048
N_WIDE = 8


def draw_neighbours(key, part):
    block_count = ATOMS // ATOM_DEV
    side_key, position_key = jax.random.split(jax.random.fold_in(key, 11))
    home_block = (jnp.arange(ATOMS, dtype=jnp.int32) // ATOM_DEV)[:, None]
    offset_step = jax.random.randint(side_key, (ATOMS, NEIGH), -1, 2)
    position = jax.random.randint(position_key, (ATOMS, NEIGH), 0, ATOM_DEV)
    return ((home_block + offset_step + block_count) % block_count * ATOM_DEV + position).astype(jnp.int32)


def with_ends(values, rng, low, high):
    dims = values.shape
    index_at = [jax.random.randint(jax.random.fold_in(rng, axis), (), 0, dims[axis]) for axis in range(len(dims))]
    values = values.at[tuple(index_at)].set(low)
    longest = dims.index(max(dims))
    index_at[longest] = (index_at[longest] + 1) % dims[longest]
    return values.at[tuple(index_at)].set(high)


def block_levels(own_key, shape, cuts, least, top_value):
    factor_of = 1.0
    for dim, parts in cuts:
        steps = jax.random.uniform(jax.random.fold_in(jax.random.fold_in(own_key, 6), dim), (parts,), jnp.float32, least / len(cuts), top_value / len(cuts))
        factor_of = factor_of * jnp.repeat(jnp.exp(steps), shape[dim] // parts).reshape((-1,) + (1,) * (len(shape) - 1 - dim))
    return factor_of


def noise(own_key, dims, spread, most, cuts=(), kind=jnp.bfloat16):
    factor_of = block_levels(own_key, dims, cuts, -0.22, 0.18) if cuts else 1.0
    array = jax.random.normal(own_key, dims, jnp.float32) * spread * factor_of
    return jnp.minimum(jnp.maximum(array, -most), most).astype(kind)


def setup_inputs(seed: int = 0) -> dict:
    key_list = jax.random.split(jax.random.key(seed), 12)
    return {
        "node_features": noise(key_list[0], (ATOMS, 25, C), 1.0, 6.0, ((0, 32),)),
        "frames": noise(key_list[1], (ATOMS, NEIGH, 165), 0.45, 6.0, ((0, 32),)),
        "radial": jnp.clip(jnp.exp(math.log(3.0) - 2.306499 * jax.random.uniform(key_list[2], (ATOMS, NEIGH, C), jnp.float32) ** block_levels(key_list[2], (ATOMS, NEIGH, C), ((0, 32),), -0.2, 0.2)), 0.29882812, 3.0).astype(jnp.bfloat16),
        "neighbours": draw_neighbours(jax.random.fold_in(key_list[11], 71), 0),
        "counts": with_ends(jax.random.randint(key_list[4], (ATOMS,), NEIGH // 3, NEIGH + 1), jax.random.fold_in(key_list[4], 1), NEIGH // 3, NEIGH).astype(jnp.int32),
        "coefficients": jnp.clip(jnp.exp(math.log(0.5) - 2.3025851 * jax.random.uniform(key_list[5], (EXPERTS,), jnp.float32) ** block_levels(key_list[5], (EXPERTS,), ((0, 8),), -0.2, 0.2)), 0.05, 0.5),
        "w_zero": noise(key_list[6], (EXPERTS, 5 * C, 5 * C), (5 * C) ** -0.5, 0.25, ((0, 8),)),
        "w_one": noise(key_list[7], (EXPERTS, 2, 4 * C, 4 * C), (8 * C) ** -0.5, 0.1875, ((0, 8),)),
        "w_two": noise(key_list[8], (EXPERTS, 2, 3 * C, 3 * C), (6 * C) ** -0.5, 0.21875, ((0, 8),)),
        "w_three": noise(key_list[9], (EXPERTS, 2, 2 * C, 2 * C), (4 * C) ** -0.5, 0.25, ((0, 8),)),
        "w_four": noise(key_list[10], (EXPERTS, 2, C, C), (2 * C) ** -0.5, 0.375, ((0, 8),)),
    }


def rotate(frames, features, inverse):
    pieces = []
    offset = 0
    for degree in range(5):
        order_size = 2 * degree + 1
        frame_block = frames[:, offset:offset + order_size * order_size].reshape(-1, order_size, order_size).astype(jnp.float32)
        component = features[:, degree * degree:degree * degree + order_size, :].astype(jnp.float32)
        if inverse:
            pieces.append(jnp.einsum('rji,rjc->ric', frame_block, component, precision=lax.Precision.HIGHEST))
        else:
            pieces.append(jnp.einsum('rij,rjc->ric', frame_block, component, precision=lax.Precision.HIGHEST))
        offset += order_size * order_size
    return jnp.concatenate(pieces, axis=1)

def convolve(rotated, merged):
    row_count = rotated.shape[0]
    channels = rotated.shape[2]
    outputs = [None] * 25
    central = jnp.stack([rotated[:, degree * degree + degree] for degree in range(5)], axis=1).reshape(row_count, 5 * channels)
    result = jnp.dot(central, merged[0], preferred_element_type=jnp.float32).reshape(row_count, 5, channels)
    for degree in range(5):
        outputs[degree * degree + degree] = result[:, degree]
    for order in range(1, 5):
        kept = 5 - order
        plus = jnp.stack([rotated[:, degree * degree + degree + order] for degree in range(order, 5)], axis=1).reshape(row_count, kept * channels)
        minus = jnp.stack([rotated[:, degree * degree + degree - order] for degree in range(order, 5)], axis=1).reshape(row_count, kept * channels)
        stacked = jnp.concatenate([plus, minus], axis=0)
        weight_pair = merged[order]
        real_part = jnp.dot(stacked, weight_pair[0], preferred_element_type=jnp.float32)
        imag_part = jnp.dot(stacked, weight_pair[1], preferred_element_type=jnp.float32)
        out_plus = (real_part[:row_count] - imag_part[row_count:]).reshape(row_count, kept, channels)
        out_minus = (real_part[row_count:] + imag_part[:row_count]).reshape(row_count, kept, channels)
        for column, degree in enumerate(range(order, 5)):
            outputs[degree * degree + degree + order] = out_plus[:, column]
            outputs[degree * degree + degree - order] = out_minus[:, column]
    return jnp.stack(outputs, axis=1)

def messages(gathered, frames, radial, merged):
    rotated = (rotate(frames, gathered, False) * radial.astype(jnp.float32)[:, None, :]).astype(jnp.bfloat16)
    mixed = convolve(rotated, merged)
    scalar = mixed[:, 0:1, :]
    gated = jnp.concatenate([jax.nn.silu(scalar), mixed[:, 1:, :] * jax.nn.sigmoid(scalar)], axis=1)
    return rotate(frames, gated, True)

def merge_weights(coefficients, weights):
    grouped_coeff = coefficients.reshape(N_WIDE, -1)
    grouped = weights.astype(jnp.float32).reshape((N_WIDE, grouped_coeff.shape[1]) + weights.shape[1:])
    partials = jnp.einsum('ge,ge...->g...', grouped_coeff, grouped, precision=lax.Precision.HIGHEST).astype(jnp.bfloat16)
    partials = lax.optimization_barrier(partials)
    return lax.optimization_barrier(jnp.sum(partials.astype(jnp.float32), axis=0)).astype(jnp.bfloat16)

def reference(node_features, frames, radial, neighbours, counts, coefficients, w_zero, w_one, w_two, w_three, w_four):
    merged = tuple((merge_weights(coefficients, weights) for weights in (w_zero, w_one, w_two, w_three, w_four)))
    atoms_total = node_features.shape[0]
    channels = node_features.shape[2]
    block_count = atoms_total // ATOM_DEV
    live_slots = (lax.broadcasted_iota(jnp.int32, neighbours.shape, 1) < counts[:, None]).astype(jnp.float32)

    def one_block(inputs):
        index_block, frame_block, radial_block, live_block = inputs
        gathered = jnp.take(node_features, index_block.reshape(-1), axis=0)
        result = messages(gathered, frame_block.reshape(-1, 165), radial_block.reshape(-1, channels), merged)
        result = result.reshape(ATOM_DEV, NEIGH, 25, channels)
        return lax.optimization_barrier(jnp.sum(result * live_block[:, :, None, None], axis=1))
    summed = lax.map(one_block, (neighbours.reshape(block_count, ATOM_DEV, NEIGH), frames.reshape(block_count, ATOM_DEV, NEIGH, 165), radial.reshape(block_count, ATOM_DEV, NEIGH, channels), live_slots.reshape(block_count, ATOM_DEV, NEIGH)))
    summed = summed.reshape(atoms_total, 25, channels)
    return summed / jnp.sqrt(counts.astype(jnp.float32))[:, None, None]
```

```python
import functools

import jax
import jax.numpy as jnp
import numpy as np
from jax import lax
from jax.experimental import pallas as pl
from jax.experimental.pallas import tpu as pltpu
from jax.sharding import PartitionSpec as P

DEGREES = 5
COMPONENTS = DEGREES * DEGREES
AXES = ("wide", "narrow")


def halo(cells):
    count = lax.axis_size(AXES)
    below = lax.ppermute(cells, AXES, [(i, (i + 1) % count) for i in range(count)])
    above = lax.ppermute(cells, AXES, [((i + 1) % count, i) for i in range(count)])
    return jnp.concatenate([below, cells, above], axis=0)


def flat_rows(weights):
    return weights.reshape(weights.shape[0], -1, weights.shape[-1])


def merge_weights(coefficients, stacks):
    members = lax.axis_size("narrow")
    member = lax.axis_index("narrow")
    pieces = []
    for weights in stacks:
        weights = flat_rows(weights)
        rows = weights.shape[1] // members
        mine = lax.dynamic_slice_in_dim(weights, member * rows, rows, 1)
        total = coefficients[0] * mine[0].astype(jnp.float32)
        for expert in range(1, weights.shape[0]):
            total = total + coefficients[expert] * mine[expert].astype(jnp.float32)
        total = total.astype(jnp.bfloat16)
        for block in range(total.shape[1] // 128):
            pieces.append(total[:, block * 128 : (block + 1) * 128])
    rows = sum(piece.shape[0] for piece in pieces)
    unit = 16 * lax.axis_size("wide")
    pieces.append(jnp.zeros((-rows % unit, 128), jnp.bfloat16))
    partial = jnp.concatenate(pieces, axis=0)
    share = lax.psum_scatter(partial, "wide", scatter_dimension=0, tiled=True)
    gathered = lax.all_gather(share, ("narrow", "wide"), axis=0, tiled=True)
    return gathered.reshape(members, -1, 128)


def conv_kernel(
    shapes,
    index_ref,
    live_ref,
    frames_ref,
    radial_ref,
    features_ref,
    merged_ref,
    scale_ref,
    out_ref,
    source_ref,
    turned_ref,
    gated_ref,
    frame_ref,
    total_ref,
    *weight_refs,
):
    step = pl.program_id(0)
    channels = radial_ref.shape[0]
    lanes = index_ref.shape[1]
    atoms = out_ref.shape[0]
    extended = features_ref.shape[1]
    members = merged_ref.shape[0]

    @pl.when(step == 0)
    def _():
        total_ref[...] = jnp.zeros_like(total_ref)
        offset = 0
        for weight_ref, (rows, columns) in zip(weight_refs, shapes):
            part = rows // members
            for block in range(columns // 128):
                whole = jnp.concatenate(
                    [merged_ref[m, pl.ds(offset, part), :] for m in range(members)], axis=0
                )
                weight_ref[pl.ds(block * 128, 128), :] = jnp.transpose(whole)
                offset += part

    for k in range(frames_ref.shape[0]):
        row = frames_ref[pl.ds(k, 1), :]
        frame_ref[k] = jnp.broadcast_to(row, (16, lanes)).astype(jnp.bfloat16)

    picked = (
        lax.broadcasted_iota(jnp.int32, (extended, lanes), 0) == index_ref[...]
    ).astype(jnp.bfloat16)

    for component in range(COMPONENTS):
        block = pl.ds(component * channels, channels)
        source_ref[block, :] = jnp.dot(
            features_ref[block, :], picked, preferred_element_type=jnp.float32
        ).astype(jnp.bfloat16)

    starts = []
    start = 0
    for order in range(DEGREES):
        starts.append(start)
        start += (DEGREES - order) * (1 if order == 0 else 2)

    row_tiles = channels // 16
    lane_tiles = lanes // 128

    def rotate(i, carried):
        row = pl.multiple_of((i // lane_tiles) * 16, 16)
        lane = pl.ds(pl.multiple_of((i % lane_tiles) * 128, 128), 128)
        radial = radial_ref[pl.ds(row, 16), lane]
        offset = 0
        for degree in range(DEGREES):
            size = 2 * degree + 1
            xs = [
                source_ref[
                    pl.ds(pl.multiple_of((degree * degree + q) * channels + row, 16), 16), lane
                ]
                for q in range(size)
            ]
            for p in range(size):
                value = frame_ref[offset + p * size, :, lane] * xs[0]
                for q in range(1, size):
                    value = value + frame_ref[offset + p * size + q, :, lane] * xs[q]
                value = value * radial
                order = abs(p - degree)
                kept = DEGREES - order
                place = starts[order] + degree - order
                if order == 0:
                    turned_ref[0, pl.ds(pl.multiple_of(place * channels + row, 16), 16), lane] = value
                else:
                    upper = pl.ds(pl.multiple_of(place * channels + row, 16), 16)
                    lower = pl.ds(pl.multiple_of((place + kept) * channels + row, 16), 16)
                    if p > degree:
                        turned_ref[0, upper, lane] = value
                        turned_ref[1, lower, lane] = value
                    else:
                        turned_ref[0, lower, lane] = -value
                        turned_ref[1, upper, lane] = value
            offset += size * size
        return carried

    lax.fori_loop(0, row_tiles * lane_tiles, rotate, 0)

    central = jnp.dot(
        weight_refs[0][...],
        turned_ref[0, pl.ds(0, DEGREES * channels), :],
        preferred_element_type=jnp.float32,
    )
    scalar = central[:channels]
    gate = live_ref[...] / (1.0 + jnp.exp(-scalar))
    for degree in range(DEGREES):
        gated_ref[pl.ds((degree * degree + degree) * channels, channels), :] = (
            central[degree * channels : (degree + 1) * channels] * gate
        ).astype(jnp.bfloat16)
    for order in range(1, DEGREES):
        kept = DEGREES - order
        span = pl.ds(starts[order] * channels, 2 * kept * channels)
        for side in range(2):
            mixed = jnp.dot(
                weight_refs[order][...],
                turned_ref[side, span, :],
                preferred_element_type=jnp.float32,
            )
            for column in range(kept):
                degree = order + column
                component = degree * degree + degree + (order if side == 0 else -order)
                gated_ref[pl.ds(component * channels, channels), :] = (
                    mixed[column * channels : (column + 1) * channels] * gate
                ).astype(jnp.bfloat16)

    def unrotate(i, carried):
        row = pl.multiple_of(i * 16, 16)
        offset = 0
        for degree in range(DEGREES):
            size = 2 * degree + 1
            sums = [None] * size
            for tile in range(lane_tiles):
                lane = pl.ds(tile * 128, 128)
                ys = [
                    gated_ref[
                        pl.ds(pl.multiple_of((degree * degree + q) * channels + row, 16), 16), lane
                    ]
                    for q in range(size)
                ]
                for p in range(size):
                    value = frame_ref[offset + p, :, lane] * ys[0]
                    for q in range(1, size):
                        value = value + frame_ref[offset + q * size + p, :, lane] * ys[q]
                    value = value.astype(jnp.float32)
                    sums[p] = value if sums[p] is None else sums[p] + value
            for p in range(size):
                place = pl.ds(pl.multiple_of((degree * degree + p) * channels + row, 16), 16)
                total_ref[place, :] = total_ref[place, :] + sums[p]
            offset += size * size
        return carried

    lax.fori_loop(0, row_tiles, unrotate, 0)

    @pl.when(step == pl.num_programs(0) - 1)
    def _():
        for component in range(COMPONENTS):
            block = jnp.transpose(total_ref[pl.ds(component * channels, channels), :])
            total = block[:atoms]
            for part in range(1, 128 // atoms):
                total = total + block[part * atoms : (part + 1) * atoms]
            out_ref[:, component, :] = total * scale_ref[...]


def body(
    node_features,
    frames,
    radial,
    neighbours,
    counts,
    coefficients,
    w_zero,
    w_one,
    w_two,
    w_three,
    w_four,
):
    atoms, components, channels = node_features.shape
    slots = neighbours.shape[1]
    entries = frames.shape[2]
    edges = atoms * slots
    stacks = (w_zero, w_one, w_two, w_three, w_four)
    merged = merge_weights(coefficients, stacks)
    shapes = [(int(np.prod(w.shape[1:-1])), w.shape[-1]) for w in stacks]

    features = halo(node_features).reshape(3 * atoms, components * channels).T
    block_start = lax.axis_index(AXES) * atoms
    atoms_total = atoms * lax.axis_size(AXES)
    index = ((neighbours - block_start + atoms) % atoms_total).T.reshape(1, edges)
    live = (lax.broadcasted_iota(jnp.int32, (slots, atoms), 0) < counts[None, :]).astype(
        jnp.float32
    ).reshape(1, edges)
    frames_t = frames.transpose(2, 1, 0).reshape(entries, edges).astype(jnp.float32)
    radial_t = radial.transpose(2, 1, 0).reshape(channels, edges)
    scale = jnp.broadcast_to(
        (1.0 / jnp.sqrt(counts.astype(jnp.float32)))[:, None], (atoms, channels)
    )

    lanes = 256
    whole = lambda shape: pl.BlockSpec(shape, lambda i: (0,) * len(shape))
    columns = lambda rows: pl.BlockSpec((rows, lanes), lambda i: (0, i))
    return pl.pallas_call(
        functools.partial(conv_kernel, shapes),
        grid=(edges // lanes,),
        in_specs=[
            columns(1),
            columns(1),
            columns(entries),
            columns(channels),
            whole(features.shape),
            whole(merged.shape),
            whole(scale.shape),
        ],
        out_specs=whole((atoms, components, channels)),
        out_shape=jax.ShapeDtypeStruct((atoms, components, channels), jnp.float32),
        scratch_shapes=[
            pltpu.VMEM((components * channels, lanes), jnp.bfloat16),
            pltpu.VMEM((2, (2 * components - DEGREES) * channels, lanes), jnp.bfloat16),
            pltpu.VMEM((components * channels, lanes), jnp.bfloat16),
            pltpu.VMEM((entries, 16, lanes), jnp.bfloat16),
            pltpu.VMEM((components * channels, 128), jnp.float32),
        ]
        + [pltpu.VMEM((n, k), jnp.bfloat16) for k, n in shapes],
        compiler_params=pltpu.CompilerParams(
            dimension_semantics=("arbitrary",), vmem_limit_bytes=56 * 1024 * 1024
        ),
    )(index, live, frames_t, radial_t, features, merged, scale)


def solution(mesh):
    spread = lambda rest: P(AXES, *([None] * rest))
    in_specs = (
        spread(2),
        spread(2),
        spread(2),
        spread(1),
        spread(0),
        P("wide"),
        P("wide", None, None),
        P("wide", None, None, None),
        P("wide", None, None, None),
        P("wide", None, None, None),
        P("wide", None, None, None),
    )
    return jax.shard_map(body, mesh=mesh, in_specs=in_specs, out_specs=spread(2), check_vma=False)
```

```python
import functools

import jax
import jax.numpy as jnp
import numpy as np
from jax import lax
from jax.experimental import pallas as pl
from jax.experimental.pallas import tpu as pltpu
from jax.sharding import PartitionSpec as P

DEGREES = 5
COMPONENTS = DEGREES * DEGREES
AXES = ("wide", "narrow")


def flat_rows(weights):
    return weights.reshape(weights.shape[0], -1, weights.shape[-1])


def exchange_kernel(
    sizes,
    coefficient_ref,
    features_ref,
    *refs,
):
    wide, narrow, count = sizes
    stacks = refs[:count]
    sides_ref, share_ref = refs[count : count + 2]
    staged = refs[count + 2 : 2 * count + 2]
    partial_ref, received_ref, load_sem, halo_send, halo_recv, send_sem, recv_sem = refs[
        2 * count + 2 :
    ]
    my_wide = lax.axis_index("wide")
    my_narrow = lax.axis_index("narrow")
    part = partial_ref.shape[0] // wide

    loads = []
    for at, (stack, stage) in enumerate(zip(stacks, staged)):
        rows = stage.shape[1]
        loads.append(
            pltpu.make_async_copy(
                stack.at[:, pl.ds(pl.multiple_of(my_narrow * rows, 16), rows), :],
                stage,
                load_sem.at[at],
            )
        )
        loads[-1].start()

    total = wide * narrow
    me = my_wide * narrow + my_narrow
    after = lax.rem(me + 1, total)
    before = lax.rem(me + total - 1, total)
    place = lambda flat: (flat // narrow, lax.rem(flat, narrow))
    peers = [(lax.rem(my_wide + hop, wide), my_narrow) for hop in range(1, wide)]
    barrier = pltpu.get_barrier_semaphore()
    for device in [place(after), place(before)] + peers:
        pl.semaphore_signal(
            barrier, inc=1, device_id=device, device_id_type=pl.DeviceIdType.MESH
        )
    pl.semaphore_wait(barrier, wide + 1)

    copies = []
    for side, device in enumerate([place(after), place(before)]):
        copies.append(
            pltpu.make_async_remote_copy(
                src_ref=features_ref,
                dst_ref=sides_ref.at[side],
                send_sem=halo_send.at[side],
                recv_sem=halo_recv.at[side],
                device_id=device,
                device_id_type=pl.DeviceIdType.MESH,
            )
        )

    offset = 0
    for load, stage in zip(loads, staged):
        load.wait()
        experts, rows, columns = stage.shape
        for block in range(columns // 128):
            lanes = pl.ds(block * 128, 128)
            value = coefficient_ref[0] * stage[0, :, lanes].astype(jnp.float32)
            for expert in range(1, experts):
                value = value + coefficient_ref[expert] * stage[expert, :, lanes].astype(
                    jnp.float32
                )
            partial_ref[pl.ds(offset, rows), :] = value.astype(jnp.bfloat16)
            offset += rows
    if offset < partial_ref.shape[0]:
        rest = partial_ref.shape[0] - offset
        partial_ref[pl.ds(offset, rest), :] = jnp.zeros((rest, 128), jnp.bfloat16)

    for hop, device in enumerate(peers):
        target = device[0]
        copies.append(
            pltpu.make_async_remote_copy(
                src_ref=partial_ref.at[pl.ds(pl.multiple_of(target * part, 16), part), :],
                dst_ref=received_ref.at[hop],
                send_sem=send_sem.at[hop],
                recv_sem=recv_sem.at[hop],
                device_id=device,
                device_id_type=pl.DeviceIdType.MESH,
            )
        )
    for copy in copies[2:]:
        copy.start()
    for copy in copies[:2]:
        copy.start()
    for copy in copies[2:]:
        copy.wait()
    summed = partial_ref[pl.ds(pl.multiple_of(my_wide * part, 16), part), :].astype(jnp.float32)
    for hop in range(wide - 1):
        summed = summed + received_ref[hop].astype(jnp.float32)
    share_ref[...] = summed.astype(jnp.bfloat16)
    for copy in copies[:2]:
        copy.wait()


def exchange(features, coefficients, stacks):
    wide = lax.axis_size("wide")
    narrow = lax.axis_size("narrow")
    stacks = [flat_rows(w) for w in stacks]
    staged = [(w.shape[0], w.shape[1] // narrow, w.shape[2]) for w in stacks]
    rows = sum(shape[1] * shape[2] // 128 for shape in staged)
    unit = 16 * wide
    rows = -(-rows // unit) * unit
    anywhere = pl.BlockSpec(memory_space=pl.ANY)
    return pl.pallas_call(
        functools.partial(exchange_kernel, (wide, narrow, len(stacks))),
        in_specs=[pl.BlockSpec(memory_space=pltpu.SMEM)] + [anywhere] * (1 + len(stacks)),
        out_specs=[anywhere, pl.BlockSpec(memory_space=pltpu.VMEM)],
        out_shape=[
            jax.ShapeDtypeStruct((2,) + features.shape, features.dtype),
            jax.ShapeDtypeStruct((rows // wide, 128), jnp.bfloat16),
        ],
        scratch_shapes=[pltpu.VMEM(shape, jnp.bfloat16) for shape in staged]
        + [
            pltpu.VMEM((rows, 128), jnp.bfloat16),
            pltpu.VMEM((wide - 1, rows // wide, 128), jnp.bfloat16),
            pltpu.SemaphoreType.DMA((len(stacks),)),
            pltpu.SemaphoreType.DMA((2,)),
            pltpu.SemaphoreType.DMA((2,)),
            pltpu.SemaphoreType.DMA((wide - 1,)),
            pltpu.SemaphoreType.DMA((wide - 1,)),
        ],
        compiler_params=pltpu.CompilerParams(collective_id=0, has_side_effects=True),
        cost_estimate=pl.CostEstimate(flops=10**9, bytes_accessed=10**7, transcendentals=0),
    )(coefficients, features, *stacks)


def order_starts():
    starts = []
    start = 0
    for order in range(DEGREES):
        starts.append(start)
        start += (DEGREES - order) * (1 if order == 0 else 2)
    return starts


def spread_frames(frames_ref, frame_ref):
    for k in range(frames_ref.shape[0]):
        row = frames_ref[pl.ds(k, 1), :]
        frame_ref[k] = jnp.broadcast_to(row, frame_ref.shape[1:]).astype(jnp.bfloat16)


def rotate_kernel(index_ref, frames_ref, radial_ref, features_ref, turned_ref, source_ref, frame_ref):
    channels, lanes = radial_ref.shape
    extended = features_ref.shape[1]
    spread_frames(frames_ref, frame_ref)

    picked = (
        lax.broadcasted_iota(jnp.int32, (extended, lanes), 0) == index_ref[...]
    ).astype(jnp.bfloat16)
    for component in range(COMPONENTS):
        block = pl.ds(component * channels, channels)
        source_ref[block, :] = jnp.dot(
            features_ref[block, :], picked, preferred_element_type=jnp.float32
        ).astype(jnp.bfloat16)

    starts = order_starts()
    lane_tiles = lanes // 128

    def rotate(i, carried):
        row = pl.multiple_of((i // lane_tiles) * 16, 16)
        lane = pl.ds(pl.multiple_of((i % lane_tiles) * 128, 128), 128)
        tile = lambda place: pl.ds(pl.multiple_of(place * channels + row, 16), 16)
        radial = radial_ref[pl.ds(row, 16), lane]
        offset = 0
        for degree in range(DEGREES):
            size = 2 * degree + 1
            xs = [source_ref[tile(degree * degree + q), lane] for q in range(size)]
            for p in range(size):
                value = frame_ref[offset + p * size, :, lane] * xs[0]
                for q in range(1, size):
                    value = value + frame_ref[offset + p * size + q, :, lane] * xs[q]
                order = abs(p - degree)
                place = starts[order] + degree - order
                if p < degree:
                    place += DEGREES - order
                turned_ref[tile(place), lane] = value * radial
            offset += size * size
        return carried

    lax.fori_loop(0, (channels // 16) * lane_tiles, rotate, 0)


def mix_kernel(
    shapes,
    live_ref,
    frames_ref,
    turned_ref,
    merged_ref,
    scale_ref,
    out_ref,
    gated_ref,
    frame_ref,
    total_ref,
    *weight_refs,
):
    step = pl.program_id(0)
    atoms, _, channels = out_ref.shape
    lanes = live_ref.shape[1]
    members = merged_ref.shape[0]
    lane_tiles = lanes // 128
    starts = order_starts()

    @pl.when(step == 0)
    def _():
        total_ref[...] = jnp.zeros_like(total_ref)
        offset = 0
        for weight_ref, (rows, columns) in zip(weight_refs, shapes):
            part = rows // members
            for block in range(columns // 128):
                whole = jnp.concatenate(
                    [merged_ref[m, pl.ds(offset, part), :] for m in range(members)], axis=0
                )
                weight_ref[pl.ds(block * 128, 128), :] = jnp.transpose(whole)
                offset += part

    spread_frames(frames_ref, frame_ref)

    central = jnp.dot(
        weight_refs[0][...],
        turned_ref[pl.ds(0, DEGREES * channels), :],
        preferred_element_type=jnp.float32,
    )
    scalar = central[:channels]
    gate = live_ref[...] / (1.0 + jnp.exp(-scalar))
    for degree in range(DEGREES):
        gated_ref[pl.ds((degree * degree + degree) * channels, channels), :] = (
            central[degree * channels : (degree + 1) * channels] * gate
        ).astype(jnp.bfloat16)
    for order in range(1, DEGREES):
        kept = DEGREES - order
        height = kept * channels
        plus = turned_ref[pl.ds(starts[order] * channels, height), :]
        minus = turned_ref[pl.ds(starts[order] * channels + height, height), :]
        for side in range(2):
            pair = [plus, -minus] if side == 0 else [minus, plus]
            mixed = jnp.dot(
                weight_refs[order][...],
                jnp.concatenate(pair, axis=0),
                preferred_element_type=jnp.float32,
            )
            for column in range(kept):
                degree = order + column
                component = degree * degree + degree + (order if side == 0 else -order)
                gated_ref[pl.ds(component * channels, channels), :] = (
                    mixed[column * channels : (column + 1) * channels] * gate
                ).astype(jnp.bfloat16)

    def unrotate(i, carried):
        row = pl.multiple_of(i * 16, 16)
        offset = 0
        for degree in range(DEGREES):
            size = 2 * degree + 1
            sums = [None] * size
            for tile in range(lane_tiles):
                lane = pl.ds(tile * 128, 128)
                ys = [
                    gated_ref[
                        pl.ds(pl.multiple_of((degree * degree + q) * channels + row, 16), 16), lane
                    ]
                    for q in range(size)
                ]
                for p in range(size):
                    value = frame_ref[offset + p, :, lane] * ys[0]
                    for q in range(1, size):
                        value = value + frame_ref[offset + q * size + p, :, lane] * ys[q]
                    value = value.astype(jnp.float32)
                    sums[p] = value if sums[p] is None else sums[p] + value
            for p in range(size):
                place = pl.ds(pl.multiple_of((degree * degree + p) * channels + row, 16), 16)
                total_ref[place, :] = total_ref[place, :] + sums[p]
            offset += size * size
        return carried

    lax.fori_loop(0, channels // 16, unrotate, 0)

    @pl.when(step == pl.num_programs(0) - 1)
    def _():
        for component in range(COMPONENTS):
            block = jnp.transpose(total_ref[pl.ds(component * channels, channels), :])
            total = block[:atoms]
            for part in range(1, 128 // atoms):
                total = total + block[part * atoms : (part + 1) * atoms]
            out_ref[:, component, :] = total * scale_ref[...]


def body(
    node_features,
    frames,
    radial,
    neighbours,
    counts,
    coefficients,
    w_zero,
    w_one,
    w_two,
    w_three,
    w_four,
):
    atoms, components, channels = node_features.shape
    slots = neighbours.shape[1]
    entries = frames.shape[2]
    edges = atoms * slots
    stacks = (w_zero, w_one, w_two, w_three, w_four)
    sides, share = exchange(node_features, coefficients, stacks)
    merged = lax.all_gather(share, ("narrow", "wide"), axis=0, tiled=True)
    merged = merged.reshape(lax.axis_size("narrow"), -1, 128)
    shapes = [(int(np.prod(w.shape[1:-1])), w.shape[-1]) for w in stacks]

    features = jnp.concatenate([sides[0], node_features, sides[1]], axis=0)
    features = features.reshape(3 * atoms, components * channels).T
    block_start = lax.axis_index(AXES) * atoms
    atoms_total = atoms * lax.axis_size(AXES)
    index = ((neighbours - block_start + atoms) % atoms_total).T.reshape(1, edges)
    live = (lax.broadcasted_iota(jnp.int32, (slots, atoms), 0) < counts[None, :]).astype(
        jnp.float32
    ).reshape(1, edges)
    frames_t = frames.transpose(2, 1, 0).reshape(entries, edges).astype(jnp.float32)
    radial_t = radial.transpose(2, 1, 0).reshape(channels, edges)
    scale = jnp.broadcast_to(
        (1.0 / jnp.sqrt(counts.astype(jnp.float32)))[:, None], (atoms, channels)
    )

    lanes = 256
    whole = lambda shape: pl.BlockSpec(shape, lambda i: (0,) * len(shape))
    columns = lambda rows: pl.BlockSpec((rows, lanes), lambda i: (0, i))
    params = pltpu.CompilerParams(
        dimension_semantics=("arbitrary",), vmem_limit_bytes=56 * 1024 * 1024
    )
    turned = pl.pallas_call(
        rotate_kernel,
        grid=(edges // lanes,),
        in_specs=[columns(1), columns(entries), columns(channels), whole(features.shape)],
        out_specs=columns(components * channels),
        out_shape=jax.ShapeDtypeStruct((components * channels, edges), jnp.bfloat16),
        scratch_shapes=[
            pltpu.VMEM((components * channels, lanes), jnp.bfloat16),
            pltpu.VMEM((entries, 16, lanes), jnp.bfloat16),
        ],
        compiler_params=params,
        cost_estimate=pl.CostEstimate(
            flops=2 * 3 * atoms * components * channels * edges,
            bytes_accessed=2 * components * channels * edges,
            transcendentals=0,
        ),
    )(index, frames_t, radial_t, features)
    return pl.pallas_call(
        functools.partial(mix_kernel, shapes),
        grid=(edges // lanes,),
        in_specs=[
            columns(1),
            columns(entries),
            columns(components * channels),
            whole(merged.shape),
            whole(scale.shape),
        ],
        out_specs=whole((atoms, components, channels)),
        out_shape=jax.ShapeDtypeStruct((atoms, components, channels), jnp.float32),
        scratch_shapes=[
            pltpu.VMEM((components * channels, lanes), jnp.bfloat16),
            pltpu.VMEM((entries, 16, lanes), jnp.bfloat16),
            pltpu.VMEM((components * channels, 128), jnp.float32),
        ]
        + [pltpu.VMEM((n, k), jnp.bfloat16) for k, n in shapes],
        compiler_params=params,
    )(live, frames_t, turned, merged, scale)


def solution(mesh):
    spread = lambda rest: P(AXES, *([None] * rest))
    in_specs = (
        spread(2),
        spread(2),
        spread(2),
        spread(1),
        spread(0),
        P("wide"),
        P("wide", None, None),
        P("wide", None, None, None),
        P("wide", None, None, None),
        P("wide", None, None, None),
        P("wide", None, None, None),
    )
    return jax.shard_map(body, mesh=mesh, in_specs=in_specs, out_specs=spread(2), check_vma=False)
```
